32 devices in a mesh: row: 4 (over z), col: 4 (over x, core), rep: 2 (over y).
Axes of the slice: x: 2, y: 2, z: 4, core: 2. Of those that a mesh axis runs over, the one named last changes fastest.
Arguments:
- a_blocks: bfloat16 [8192, 1024], P('row', 'col'), may hold values from -6 to 6
- a_mask: int32 [32, 4], P('row', 'col'), may hold values from 0 to 1, as said below
- b_blocks: bfloat16 [1024, 2048], P('row', 'col'), may hold values from -0.1875 to 0.1875
- b_mask: int32 [4, 8], P('row', 'col'), may hold values from 0 to 1
Outputs:
- c_product: bfloat16 [8192, 2048], P('row', ('col', 'rep'))
The draws below stay inside these ranges and needn't reach their ends.
Inputs may be any that keep to these rules, and one draw needn't show every extreme that they name: a_mask holds 0 or 1; within each aligned tile of 8 block rows by 1 inner blocks (one device's tile) at most 2 entries are 1, and some tile holds exactly 2.
All inputs are finite; a program needn't handle non-finite values.
Results may differ from the reference program's by a relative error of at most 0.007.
Values may be sent and summed in bfloat16 or wider, within the bound.
No kernel may reach another device: no remote copies, remote signals or barrier semaphores. Data moves between devices by JAX's collectives and lax.ppermute only.
A program may use at most 64 MiB of HBM per device.

```python
import jax
import jax.numpy as jnp

BS = 256
MB = 8
KA = 1
AMOST = 2
MT = 32
KT = 4
NT = 8


def draw_a_mask(key, part):
    tile_rows = MT // MB
    tile_cols = KT // KA
    tile_cells = MB * KA
    key_patch, key_sparse, key_order = jax.random.split(jax.random.fold_in(key, 11), 3)
    row_place = jnp.arange(tile_rows, dtype=jnp.int32)[:, None]
    col_place = jnp.arange(tile_cols, dtype=jnp.int32)[None, :]
    centre = row_place * tile_cols // tile_rows
    distance = jnp.abs(col_place - centre)
    distance = jnp.minimum(distance, tile_cols - distance)
    patches = jax.random.randint(key_patch, (tile_rows, tile_cols), 0, 8) == 0
    sparse_count = jax.random.randint(key_sparse, (tile_rows, tile_cols), 0, AMOST // 2 + 1)
    counts = jnp.where((distance <= 1) | patches, AMOST, sparse_count)
    scores = jax.random.randint(key_order, (tile_rows, tile_cols, tile_cells), 0, 1 << 20) * tile_cells + jnp.arange(tile_cells, dtype=jnp.int32)
    ranking = jnp.argsort(jnp.argsort(scores, axis=-1), axis=-1)
    pattern = (ranking < counts[:, :, None]).astype(jnp.int32)
    pattern = pattern.reshape(tile_rows, tile_cols, MB, KA).transpose(0, 2, 1, 3)
    return pattern.reshape(MT, KT)


def draw_b_mask(key, part):
    inner_place = jnp.arange(KT, dtype=jnp.int32)[:, None]
    column_place = jnp.arange(NT, dtype=jnp.int32)[None, :]
    centre = inner_place * NT // KT
    distance = jnp.abs(column_place - centre)
    distance = jnp.minimum(distance, NT - distance)
    drawn = jax.random.randint(jax.random.fold_in(key, 23), (KT, NT), 0, 20)
    pattern = jnp.where(distance * 8 <= NT, drawn < 16, drawn < 3)
    return pattern.astype(jnp.int32)


def steps_of(rng, shape, shards, least, high):
    loudness, own = 1.0, jax.random.fold_in(rng, 6)
    for axis_at, blocks in shards:
        heights = jnp.exp(jax.random.uniform(jax.random.fold_in(own, axis_at), (blocks,), jnp.float32, least / len(shards), high / len(shards)))
        loudness = loudness * jnp.repeat(heights, shape[axis_at] // blocks).reshape([-1 if axis == axis_at else 1 for axis in range(len(shape))])
    return loudness


def bell_draw(key, dims, spread, reach, shards=(), kind=jnp.bfloat16):
    entries = spread * jax.random.normal(key, dims, jnp.float32)
    if shards:
        entries = entries * steps_of(key, dims, shards, -0.22, 0.18)
    return jnp.clip(entries, -reach, reach).astype(kind)


def setup_inputs(seed: int = 0) -> dict:
    arg_keys = jax.random.split(jax.random.key(seed), 5)
    return {
        "a_blocks": bell_draw(arg_keys[0], (MT * BS, KT * BS), 1.0, 6.0, ((0, 4), (1, 4))),
        "a_mask": draw_a_mask(jax.random.fold_in(arg_keys[4], 71), 0),
        "b_blocks": bell_draw(arg_keys[2], (KT * BS, NT * BS), (KT * BS) ** -0.5, 0.1875, ((0, 4), (1, 4))),
        "b_mask": draw_b_mask(jax.random.fold_in(arg_keys[4], 71), 0),
    }


def expand(values, pattern):
    block_rows = pattern.shape[0]
    block_cols = pattern.shape[1]
    shaped = values.reshape(block_rows, BS, block_cols, BS) * pattern[:, None, :, None].astype(jnp.bfloat16)
    return shaped.reshape(block_rows * BS, block_cols * BS)


def reference(a_blocks, a_mask, b_blocks, b_mask):
    masked_a = expand(a_blocks, a_mask)
    masked_b = expand(b_blocks, b_mask)
    return jnp.dot(masked_a, masked_b, preferred_element_type=jnp.float32).astype(jnp.bfloat16)
```

```python
import functools

import jax
import jax.numpy as jnp
from jax import lax
from jax.experimental import pallas as pl
from jax.experimental.pallas import tpu as pltpu
from jax.sharding import PartitionSpec as P


BS = 256
CODE_ALIGN = 16


def pack_kernel(slots, mask_ref, a_ref, out_ref, sem):
    rows, cols = mask_ref.shape
    cells = rows * cols
    place = [jnp.int32(cells)] * slots
    count = jnp.int32(0)
    for cell in range(cells):
        hit = mask_ref[cell // cols, cell % cols] == 1
        for slot in range(slots):
            place[slot] = jnp.where(hit & (count == slot), cell, place[slot])
        count = count + hit.astype(jnp.int32)
    copies = []
    for slot in range(slots):
        cell = jnp.minimum(place[slot], cells - 1)
        copies.append(
            pltpu.make_async_copy(
                a_ref.at[pl.ds((cell // cols) * BS, BS), pl.ds((cell % cols) * BS, BS)]
                if cols > 1
                else a_ref.at[pl.ds(cell * BS, BS), :],
                out_ref.at[pl.ds(slot * BS, BS), :],
                sem.at[slot],
            )
        )
        copies[-1].start()
    code_rows = out_ref.shape[0] - slots * BS
    index = lax.broadcasted_iota(jnp.int32, (code_rows, BS), 0)
    codes = jnp.full((code_rows, BS), cells, jnp.int32)
    for slot in range(slots):
        codes = jnp.where(index == slot, place[slot], codes)
    out_ref[pl.ds(slots * BS, code_rows), :] = codes.astype(jnp.float32).astype(jnp.bfloat16)
    for copy in copies:
        copy.wait()


def product_kernel(slots, inner_local, b_blocks, *refs):
    owner_ref = refs[0]
    rest = refs[1:]
    out_ref, total, stacked = rest[-3:]
    rest = rest[:-3]
    n_b = b_blocks
    a_refs, b_refs = rest[: len(rest) - n_b], rest[len(rest) - n_b :]
    rows = out_ref.shape[0]
    n_a = len(a_refs)
    cells = (rows // BS) * inner_local
    total[...] = jnp.zeros_like(total)
    depth = b_refs[0].shape[0]
    for i, b_ref in enumerate(b_refs):
        stacked[pl.ds(pl.multiple_of(owner_ref[n_a + i] * depth, depth), depth), :] = b_ref[...]
    for i, a_ref in enumerate(a_refs):
        code_rows = a_ref.shape[0] - slots * BS
        codes = a_ref[pl.ds(slots * BS, code_rows), :].astype(jnp.float32)
        index = lax.broadcasted_iota(jnp.int32, codes.shape, 0)
        for slot in range(slots):
            code = jnp.max(jnp.where(index == slot, codes, 0.0)).astype(jnp.int32)
            used = code < cells
            row = jnp.where(used, code // inner_local, rows // BS)
            inner = jnp.where(used, code % inner_local, 0) + owner_ref[i] * inner_local
            where = pl.ds(pl.multiple_of(row * BS, BS), BS)
            total[where, :] += jnp.dot(
                a_ref[pl.ds(slot * BS, BS), :],
                stacked[pl.ds(pl.multiple_of(inner * BS, BS), BS), :],
                preferred_element_type=jnp.float32,
            )
    out_ref[...] = total[pl.ds(0, rows), :].astype(jnp.bfloat16)


def exchange(values, axis, n):
    me = lax.axis_index(axis)
    held = [(values, me)]
    if n & (n - 1):
        for step in range(1, n):
            moved = lax.ppermute(values, axis, [(i, (i + step) % n) for i in range(n)])
            held.append((moved, lax.rem(me + n - step, n)))
        return held
    step = n // 2
    while step:
        pairs = [(i, i ^ step) for i in range(n)]
        held += [(lax.ppermute(v, axis, pairs), owner ^ step) for v, owner in held]
        step //= 2
    return held


def per_device(shape, a_blocks, a_mask, b_blocks, b_mask):
    own_width = b_blocks.shape[1] // shape["rep"]
    layer = lax.axis_index("rep")
    depth = b_blocks.shape[0]
    own_b = lax.dynamic_slice_in_dim(b_blocks, layer * own_width, own_width, 1)
    column_mask = jnp.repeat(b_mask, BS, axis=1)
    own_mask = lax.dynamic_slice_in_dim(column_mask, layer * own_width, own_width, 1)
    own_mask = jnp.repeat(own_mask, BS, axis=0).astype(jnp.bfloat16)
    own_b = own_b * own_mask
    row_n, col_n = shape["row"], shape["col"]
    me_row = lax.axis_index("row")
    b_held = [(own_b, me_row)]
    for step in range(1, row_n):
        moved = lax.ppermute(own_b, "row", [(i, (i + step) % row_n) for i in range(row_n)])
        b_held.append((moved, lax.rem(me_row + row_n - step, row_n)))

    rows = a_blocks.shape[0]
    block_rows, inner_local = a_mask.shape
    slots = max(block_rows // 4, 1)
    code_rows = -(-slots // CODE_ALIGN) * CODE_ALIGN
    packed = pl.pallas_call(
        functools.partial(pack_kernel, slots),
        out_shape=jax.ShapeDtypeStruct((slots * BS + code_rows, BS), jnp.bfloat16),
        in_specs=[
            pl.BlockSpec(memory_space=pltpu.SMEM),
            pl.BlockSpec(memory_space=pl.ANY),
        ],
        out_specs=pl.BlockSpec(memory_space=pltpu.VMEM),
        scratch_shapes=[pltpu.SemaphoreType.DMA((slots,))],
        compiler_params=pltpu.CompilerParams(vmem_limit_bytes=4 << 20),
        name="pack",
    )(a_mask, a_blocks)
    a_held = exchange(packed, "col", col_n)

    owners = jnp.stack([o for _, o in a_held] + [o for _, o in b_held]).astype(jnp.int32)
    return pl.pallas_call(
        functools.partial(product_kernel, slots, inner_local, row_n),
        out_shape=jax.ShapeDtypeStruct((rows, own_width), jnp.bfloat16),
        in_specs=[pl.BlockSpec(memory_space=pltpu.SMEM)]
        + [pl.BlockSpec(memory_space=pltpu.VMEM)] * (col_n + row_n),
        out_specs=pl.BlockSpec(memory_space=pltpu.VMEM),
        scratch_shapes=[
            pltpu.VMEM((rows + BS, own_width), jnp.float32),
            pltpu.VMEM((row_n * depth, own_width), jnp.bfloat16),
        ],
        compiler_params=pltpu.CompilerParams(vmem_limit_bytes=16 << 20),
        name="product",
    )(owners, *[v for v, _ in a_held], *[v for v, _ in b_held])


def solution(mesh):
    in_specs = (P("row", "col"), P("row", "col"), P("row", "col"), P("row", "col"))
    out_specs = P("row", ("col", "rep"))
    return jax.shard_map(
        functools.partial(per_device, dict(mesh.shape)),
        mesh=mesh,
        in_specs=in_specs,
        out_specs=out_specs,
        check_vma=False,
    )
```

```python
import functools

import jax
import jax.numpy as jnp
from jax import lax
from jax.experimental import pallas as pl
from jax.experimental.pallas import tpu as pltpu
from jax.sharding import PartitionSpec as P


BS = 256
CODE_ALIGN = 16


def block(index):
    start = index * BS
    return pl.ds(start if isinstance(index, int) else pl.multiple_of(start, BS), BS)


def prep_kernel(slots, rows, cols, am_ref, a_ref, bm_ref, b_ref, pack_ref, own_ref, am, bm, a_sem, b_sem, m_sem):
    width = own_ref.shape[1]
    wide = width // BS
    layer = lax.axis_index("rep")
    load_am = pltpu.make_async_copy(am_ref, am, m_sem.at[0])
    load_bm = pltpu.make_async_copy(bm_ref, bm, m_sem.at[1])
    load_b = pltpu.make_async_copy(
        b_ref.at[:, pl.ds(pl.multiple_of(layer * width, width), width)], own_ref, b_sem
    )
    load_am.start()
    load_bm.start()
    load_b.start()
    load_am.wait()
    cells = rows * cols
    place = [jnp.int32(cells)] * slots
    count = jnp.int32(0)
    for cell in range(cells):
        hit = am[cell % cols, cell // cols] == 1
        for slot in range(slots):
            place[slot] = jnp.where(hit & (count == slot), cell, place[slot])
        count = count + hit.astype(jnp.int32)
    copies = []
    for slot in range(slots):
        cell = jnp.minimum(place[slot], cells - 1)
        across = block(cell % cols) if cols > 1 else slice(None)
        copies.append(
            pltpu.make_async_copy(
                a_ref.at[block(cell // cols if cols > 1 else cell), across],
                pack_ref.at[block(slot), :],
                a_sem.at[slot],
            )
        )
        copies[-1].start()
    code_rows = pack_ref.shape[0] - slots * BS
    index = lax.broadcasted_iota(jnp.int32, (code_rows, BS), 0)
    codes = jnp.full((code_rows, BS), cells, jnp.int32)
    for slot in range(slots):
        codes = jnp.where(index == slot, place[slot], codes)
    pack_ref[pl.ds(slots * BS, code_rows), :] = codes.astype(jnp.float32).astype(jnp.bfloat16)
    load_bm.wait()
    load_b.wait()
    for down in range(own_ref.shape[0] // BS):
        for over in range(wide):
            keep = bm[down, layer * wide + over].astype(jnp.float32)
            part = (block(down), block(over))
            own_ref[part] = (own_ref[part].astype(jnp.float32) * keep).astype(jnp.bfloat16)
    for copy in copies:
        copy.wait()


def add_products(slots, inner_local, rows, a_refs, a_owners, b_refs, b_owners, total):
    cells = rows // BS * inner_local
    depth = b_refs[0].shape[0] // BS
    found = []
    for a_ref, owner in zip(a_refs, a_owners):
        codes = a_ref[pl.ds(slots * BS, CODE_ALIGN), pl.ds(0, 128)].astype(jnp.float32)
        index = lax.broadcasted_iota(jnp.int32, codes.shape, 0)
        for slot in range(slots):
            code = jnp.max(jnp.where(index == slot, codes, 0.0)).astype(jnp.int32)
            row = code // inner_local if inner_local > 1 else code
            inner = owner * inner_local + (code % inner_local if inner_local > 1 else 0)
            found.append((a_ref, slot, code < cells, row, inner))
    for a_ref, slot, used, row, inner in found:
        for b_ref, owner in zip(b_refs, b_owners):

            @pl.when(used & (inner // depth == owner))
            def _():
                inside = block(inner % depth) if depth > 1 else slice(None)
                where = block(row)
                total[where, :] += jnp.dot(
                    a_ref[block(slot), :], b_ref[inside, :], preferred_element_type=jnp.float32
                )


def early_kernel(slots, inner_local, a_of, b_of, *refs):
    a_refs, b_refs, total = refs[: len(a_of)], refs[len(a_of) : -1], refs[-1]
    total[...] = jnp.zeros_like(total)
    a_owners = [of(lax.axis_index("col")) for of in a_of]
    b_owners = [of(lax.axis_index("row")) for of in b_of]
    add_products(slots, inner_local, total.shape[0], a_refs, a_owners, b_refs, b_owners, total)


def late_kernel(slots, inner_local, a_of, b_of, total_ref, *refs):
    a_refs, b_refs = refs[: len(a_of)], refs[len(a_of) : -4]
    total, out_ref, stage, sem = refs[-4:]
    a_owners = [of(lax.axis_index("col")) for of in a_of]
    b_owners = [of(lax.axis_index("row")) for of in b_of]
    add_products(slots, inner_local, total.shape[0], a_refs, a_owners, b_refs, b_owners, total)
    copies = []
    for row in range(total.shape[0] // BS):
        stage[block(row), :] = total[block(row), :].astype(jnp.bfloat16)
        copies.append(
            pltpu.make_async_copy(stage.at[block(row), :], out_ref.at[block(row), :], sem.at[row])
        )
        copies[-1].start()
    for copy in copies:
        copy.wait()


def flip(step):
    return lambda me: me ^ step


def behind(step, n):
    return lambda me: lax.rem(me + n - step, n)


def hops(n):
    if n & (n - 1):
        return [([(i, (i + s) % n) for i in range(n)], behind(s, n)) for s in range(1, n)]
    order = list(range(n // 2, n)) + list(range(1, n // 2))
    return [([(i, i ^ s) for i in range(n)], flip(s)) for s in order]


def spread(values, axis, n):
    same = lambda me: me
    held = [(values, same)]
    if n & (n - 1):
        return held + [
            (lax.ppermute(values, axis, pairs), of) for pairs, of in hops(n)
        ]
    step = n // 2
    masks = [(values, 0)]
    while step:
        pairs = [(i, i ^ step) for i in range(n)]
        fresh = []
        for v, mask in masks:
            fresh.append((lax.ppermute(v, axis, pairs), mask ^ step))
        masks += fresh
        step //= 2
    return [(v, flip(mask)) for v, mask in masks]


VMEM = pl.BlockSpec(memory_space=pltpu.VMEM)
HBM = pl.BlockSpec(memory_space=pltpu.HBM)


def per_device(shape, a_blocks, a_mask, b_blocks, b_mask):
    row_n, col_n = shape["row"], shape["col"]
    own_width = b_blocks.shape[1] // shape["rep"]
    depth = b_blocks.shape[0]
    rows = a_blocks.shape[0]
    block_rows, inner_local = a_mask.shape
    slots = max(block_rows // 4, 1)
    code_rows = -(-slots // CODE_ALIGN) * CODE_ALIGN
    packed, own_b = pl.pallas_call(
        functools.partial(prep_kernel, slots, block_rows, inner_local),
        out_shape=[
            pltpu.VMEM((slots * BS + code_rows, BS), jnp.bfloat16),
            pltpu.VMEM((depth, own_width), jnp.bfloat16),
        ],
        in_specs=[HBM] * 4,
        out_specs=[VMEM] * 2,
        scratch_shapes=[
            pltpu.SMEM(a_mask.shape[::-1], jnp.int32),
            pltpu.SMEM(b_mask.shape, jnp.int32),
            pltpu.SemaphoreType.DMA((slots,)),
            pltpu.SemaphoreType.DMA,
            pltpu.SemaphoreType.DMA((2,)),
        ],
        compiler_params=pltpu.CompilerParams(vmem_limit_bytes=60 << 20),
        name="prep",
    )(a_mask.T, a_blocks, b_mask, b_blocks)
    b_held = [(own_b, lambda me: me)]
    for pairs, of in hops(row_n):
        b_held.append((lax.ppermute(own_b, "row", pairs), of))
    a_held = spread(packed, "col", col_n)
    far = -(-row_n // 2)
    early, late = b_held[:1] + b_held[1 + far :], b_held[1 : 1 + far]
    a_of = [of for _, of in a_held]
    total = pl.pallas_call(
        functools.partial(early_kernel, slots, inner_local, a_of, [of for _, of in early]),
        out_shape=jax.ShapeDtypeStruct((rows, own_width), jnp.float32),
        in_specs=[VMEM] * (len(a_held) + len(early)),
        out_specs=VMEM,
        compiler_params=pltpu.CompilerParams(vmem_limit_bytes=8 << 20),
        cost_estimate=pl.CostEstimate(flops=1 << 30, bytes_accessed=1 << 22, transcendentals=0),
        name="early",
    )(*[v for v, _ in a_held], *[v for v, _ in early])
    _, product = pl.pallas_call(
        functools.partial(late_kernel, slots, inner_local, a_of, [of for _, of in late]),
        out_shape=[
            jax.ShapeDtypeStruct((rows, own_width), jnp.float32),
            jax.ShapeDtypeStruct((rows, own_width), jnp.bfloat16),
        ],
        in_specs=[VMEM] * (1 + len(a_held) + len(late)),
        out_specs=[VMEM, HBM],
        scratch_shapes=[
            pltpu.VMEM((rows, own_width), jnp.bfloat16),
            pltpu.SemaphoreType.DMA((rows // BS,)),
        ],
        input_output_aliases={0: 0},
        compiler_params=pltpu.CompilerParams(vmem_limit_bytes=8 << 20),
        name="late",
    )(total, *[v for v, _ in a_held], *[v for v, _ in late])
    return product


def solution(mesh):
    in_specs = (P("row", "col"), P("row", "col"), P("row", "col"), P("row", "col"))
    out_specs = P("row", ("col", "rep"))
    return jax.shard_map(
        functools.partial(per_device, dict(mesh.shape)),
        mesh=mesh,
        in_specs=in_specs,
        out_specs=out_specs,
        check_vma=False,
    )
```

```python
import functools

import jax
import jax.numpy as jnp
from jax import lax
from jax.experimental import pallas as pl
from jax.experimental.pallas import tpu as pltpu
from jax.sharding import PartitionSpec as P


BS = 256
CODE_ALIGN = 16
LATE = (1, 2)


def block(index):
    start = index * BS
    return pl.ds(start if isinstance(index, int) else pl.multiple_of(start, BS), BS)


def prep_kernel(slots, rows, cols, am_ref, a_ref, bm_ref, b_ref, pack_ref, own_ref, am, bm, a_sem, b_sem, m_sem):
    width = own_ref.shape[1]
    wide = width // BS
    layer = lax.axis_index("rep")
    load_am = pltpu.make_async_copy(am_ref, am, m_sem.at[0])
    load_bm = pltpu.make_async_copy(bm_ref, bm, m_sem.at[1])
    load_b = pltpu.make_async_copy(
        b_ref.at[:, pl.ds(pl.multiple_of(layer * width, width), width)], own_ref, b_sem
    )
    load_am.start()
    load_bm.start()
    load_b.start()
    load_am.wait()
    cells = rows * cols
    place = [jnp.int32(cells)] * slots
    count = jnp.int32(0)
    for cell in range(cells):
        hit = am[cell % cols, cell // cols] == 1
        for slot in range(slots):
            place[slot] = jnp.where(hit & (count == slot), cell, place[slot])
        count = count + hit.astype(jnp.int32)
    copies = []
    for slot in range(slots):
        cell = jnp.minimum(place[slot], cells - 1)
        across = block(cell % cols) if cols > 1 else slice(None)
        copies.append(
            pltpu.make_async_copy(
                a_ref.at[block(cell // cols if cols > 1 else cell), across],
                pack_ref.at[block(slot), :],
                a_sem.at[slot],
            )
        )
        copies[-1].start()
    code_rows = pack_ref.shape[0] - slots * BS
    index = lax.broadcasted_iota(jnp.int32, (code_rows, BS), 0)
    codes = jnp.full((code_rows, BS), cells, jnp.int32)
    for slot in range(slots):
        codes = jnp.where(index == slot, place[slot], codes)
    pack_ref[pl.ds(slots * BS, code_rows), :] = codes.astype(jnp.float32).astype(jnp.bfloat16)
    load_bm.wait()
    load_b.wait()
    for down in range(own_ref.shape[0] // BS):
        for over in range(wide):
            keep = bm[down, layer * wide + over].astype(jnp.float32)
            part = (block(down), block(over))
            own_ref[part] = (own_ref[part].astype(jnp.float32) * keep).astype(jnp.bfloat16)
    for copy in copies:
        copy.wait()


def add_products(slots, inner_local, rows, a_refs, a_owners, b_refs, b_owners, total):
    cells = rows // BS * inner_local
    depth = b_refs[0].shape[0] // BS
    groups = []
    for a_ref, owner in zip(a_refs, a_owners):
        codes = a_ref[pl.ds(slots * BS, CODE_ALIGN), pl.ds(0, 128)].astype(jnp.float32)
        index = lax.broadcasted_iota(jnp.int32, codes.shape, 0)
        places = [
            jnp.max(jnp.where(index == slot, codes, 0.0)).astype(jnp.int32) for slot in range(slots)
        ]
        if inner_local == 1:
            groups.append((a_ref, 0, places, owner))
        else:
            for slot, place in enumerate(places):
                inside = jnp.where(place < cells, lax.rem(place, inner_local), 0)
                groups.append((a_ref, slot, [place // inner_local], owner * inner_local + inside))
    for a_ref, slot, places, inner in groups:
        for b_ref, owner in zip(b_refs, b_owners):

            @pl.when((inner // depth if depth > 1 else inner) == owner)
            def _():
                inside = block(lax.rem(inner, depth)) if depth > 1 else slice(None)
                products = jnp.dot(
                    a_ref[pl.ds(slot * BS, len(places) * BS), :],
                    b_ref[inside, :],
                    preferred_element_type=jnp.float32,
                )
                for at, row in enumerate(places):
                    total[block(row), :] += products[at * BS : (at + 1) * BS]


def early_kernel(slots, inner_local, a_of, b_of, *refs):
    a_refs, b_refs, total = refs[: len(a_of)], refs[len(a_of) : -1], refs[-1]
    total[...] = jnp.zeros_like(total)
    a_owners = [of(lax.axis_index("col")) for of in a_of]
    b_owners = [of(lax.axis_index("row")) for of in b_of]
    add_products(slots, inner_local, total.shape[0] - BS, a_refs, a_owners, b_refs, b_owners, total)


def late_kernel(slots, inner_local, a_of, b_of, total_ref, *refs):
    a_refs, b_refs = refs[: len(a_of)], refs[len(a_of) : -4]
    total, out_ref, stage, sem = refs[-4:]
    a_owners = [of(lax.axis_index("col")) for of in a_of]
    b_owners = [of(lax.axis_index("row")) for of in b_of]
    add_products(slots, inner_local, total.shape[0] - BS, a_refs, a_owners, b_refs, b_owners, total)
    copies = []
    for row in range(out_ref.shape[0] // BS):
        stage[block(row), :] = total[block(row), :].astype(jnp.bfloat16)
        copies.append(
            pltpu.make_async_copy(stage.at[block(row), :], out_ref.at[block(row), :], sem.at[row])
        )
        copies[-1].start()
    for copy in copies:
        copy.wait()


def flip(step):
    return lambda me: me ^ step


def behind(step, n):
    return lambda me: lax.rem(me + n - step, n)


def route(n):
    own = list(range(n))
    if n & (n - 1):
        steps = [([(i, (i + s) % n) for i in own], None, s > n // 2) for s in range(1, n)]
    else:
        order = list(range(n // 2, n)) + list(range(1, n // 2))
        steps = [([(i, i ^ s) for i in own], None, at in LATE) for at, s in enumerate(order)]
    plan = []
    for pairs, source, late in steps:
        holds = {i: i for i in own} if source is None else plan[source][2]
        plan.append((pairs, source, {dst: holds[src] for src, dst in pairs}, late))
    return plan


def owner_of(table):
    def of(me):
        owner = jnp.int32(-1)
        for device, held in table.items():
            owner = jnp.where(me == device, held, owner)
        return owner

    return of


def spread(values, axis, n):
    same = lambda me: me
    held = [(values, same)]
    if n & (n - 1):
        return held + [
            (lax.ppermute(values, axis, [(i, (i + s) % n) for i in range(n)]), behind(s, n))
            for s in range(1, n)
        ]
    step = n // 2
    masks = [(values, 0)]
    while step:
        pairs = [(i, i ^ step) for i in range(n)]
        fresh = []
        for v, mask in masks:
            fresh.append((lax.ppermute(v, axis, pairs), mask ^ step))
        masks += fresh
        step //= 2
    return [(v, flip(mask)) for v, mask in masks]


VMEM = pl.BlockSpec(memory_space=pltpu.VMEM)
HBM = pl.BlockSpec(memory_space=pltpu.HBM)


def per_device(shape, a_blocks, a_mask, b_blocks, b_mask):
    row_n, col_n = shape["row"], shape["col"]
    own_width = b_blocks.shape[1] // shape["rep"]
    depth = b_blocks.shape[0]
    rows = a_blocks.shape[0]
    block_rows, inner_local = a_mask.shape
    slots = max(block_rows // 4, 1)
    code_rows = -(-slots // CODE_ALIGN) * CODE_ALIGN
    packed, own_b = pl.pallas_call(
        functools.partial(prep_kernel, slots, block_rows, inner_local),
        out_shape=[
            pltpu.VMEM((slots * BS + code_rows, BS), jnp.bfloat16),
            pltpu.VMEM((depth, own_width), jnp.bfloat16),
        ],
        in_specs=[HBM] * 4,
        out_specs=[VMEM] * 2,
        scratch_shapes=[
            pltpu.SMEM(a_mask.shape[::-1], jnp.int32),
            pltpu.SMEM(b_mask.shape, jnp.int32),
            pltpu.SemaphoreType.DMA((slots,)),
            pltpu.SemaphoreType.DMA,
            pltpu.SemaphoreType.DMA((2,)),
        ],
        compiler_params=pltpu.CompilerParams(vmem_limit_bytes=60 << 20),
        name="prep",
    )(a_mask.T, a_blocks, b_mask, b_blocks)
    plan = route(row_n)
    arrived = []
    for pairs, source, _, _ in plan:
        sent = own_b if source is None else arrived[source]
        arrived.append(lax.ppermute(sent, "row", pairs))
    a_held = spread(packed, "col", col_n)
    held = [(v, owner_of(step[2]), step[3]) for v, step in zip(arrived, plan)]
    early = [(own_b, lambda me: me)] + [(v, of) for v, of, late in held if not late]
    late = [(v, of) for v, of, late in held if late]
    a_of = [of for _, of in a_held]
    total = pl.pallas_call(
        functools.partial(early_kernel, slots, inner_local, a_of, [of for _, of in early]),
        out_shape=jax.ShapeDtypeStruct((rows + BS, own_width), jnp.float32),
        in_specs=[VMEM] * (len(a_held) + len(early)),
        out_specs=VMEM,
        compiler_params=pltpu.CompilerParams(vmem_limit_bytes=8 << 20),
        cost_estimate=pl.CostEstimate(flops=1 << 30, bytes_accessed=1 << 22, transcendentals=0),
        name="early",
    )(*[v for v, _ in a_held], *[v for v, _ in early])
    _, product = pl.pallas_call(
        functools.partial(late_kernel, slots, inner_local, a_of, [of for _, of in late]),
        out_shape=[
            jax.ShapeDtypeStruct((rows + BS, own_width), jnp.float32),
            jax.ShapeDtypeStruct((rows, own_width), jnp.bfloat16),
        ],
        in_specs=[VMEM] * (1 + len(a_held) + len(late)),
        out_specs=[VMEM, HBM],
        scratch_shapes=[
            pltpu.VMEM((rows, own_width), jnp.bfloat16),
            pltpu.SemaphoreType.DMA((rows // BS,)),
        ],
        input_output_aliases={0: 0},
        compiler_params=pltpu.CompilerParams(vmem_limit_bytes=8 << 20),
        name="late",
    )(total, *[v for v, _ in a_held], *[v for v, _ in late])
    return product


def solution(mesh):
    in_specs = (P("row", "col"), P("row", "col"), P("row", "col"), P("row", "col"))
    out_specs = P("row", ("col", "rep"))
    return jax.shard_map(
        functools.partial(per_device, dict(mesh.shape)),
        mesh=mesh,
        in_specs=in_specs,
        out_specs=out_specs,
        check_vma=False,
    )
```

```python
import functools

import jax
import jax.numpy as jnp
from jax import lax
from jax.experimental import pallas as pl
from jax.experimental.pallas import tpu as pltpu
from jax.sharding import PartitionSpec as P


BS = 256
CODE_ALIGN = 16
LATE = (1, 2)


def block(index):
    start = index * BS
    return pl.ds(start if isinstance(index, int) else pl.multiple_of(start, BS), BS)


def prep_kernel(slots, rows, cols, am_ref, a_ref, bm_ref, b_ref, pack_ref, own_ref, am, bm, tile, a_sem, b_sem, m_sem):
    width = own_ref.shape[1]
    wide = width // BS
    layer = lax.axis_index("rep")
    load_am = pltpu.make_async_copy(am_ref, am, m_sem.at[0])
    load_bm = pltpu.make_async_copy(bm_ref, bm, m_sem.at[1])
    load_b = pltpu.make_async_copy(
        b_ref.at[:, pl.ds(pl.multiple_of(layer * width, width), width)], own_ref, b_sem
    )
    load_am.start()
    load_bm.start()
    load_b.start()
    load_a = pltpu.make_async_copy(a_ref, tile, a_sem)
    load_a.start()
    load_am.wait()
    cells = rows * cols
    place = [jnp.int32(cells)] * slots
    count = jnp.int32(0)
    for cell in range(cells):
        hit = am[cell % cols, cell // cols] == 1
        for slot in range(slots):
            place[slot] = jnp.where(hit & (count == slot), cell, place[slot])
        count = count + hit.astype(jnp.int32)
    load_a.wait()
    for slot in range(slots):
        cell = jnp.minimum(place[slot], cells - 1)
        if cols == 1:
            pack_ref[block(slot), :] = tile[block(cell), :]
        else:
            pack_ref[block(slot), :] = tile[block(cell // cols), block(lax.rem(cell, cols))]
    code_rows = pack_ref.shape[0] - slots * BS
    index = lax.broadcasted_iota(jnp.int32, (code_rows, BS), 0)
    codes = jnp.full((code_rows, BS), cells, jnp.int32)
    for slot in range(slots):
        codes = jnp.where(index == slot, place[slot], codes)
    pack_ref[pl.ds(slots * BS, code_rows), :] = codes.astype(jnp.float32).astype(jnp.bfloat16)
    load_bm.wait()
    load_b.wait()
    for down in range(own_ref.shape[0] // BS):
        for over in range(wide):
            keep = bm[down, layer * wide + over].astype(jnp.float32)
            part = (block(down), block(over))
            own_ref[part] = (own_ref[part].astype(jnp.float32) * keep).astype(jnp.bfloat16)


def read_places(slots, a_refs, places_ref):
    for at, a_ref in enumerate(a_refs):
        codes = a_ref[pl.ds(slots * BS, CODE_ALIGN), pl.ds(0, 128)].astype(jnp.float32)
        index = lax.broadcasted_iota(jnp.int32, codes.shape, 0)
        for slot in range(slots):
            place = jnp.max(jnp.where(index == slot, codes, 0.0)).astype(jnp.int32)
            places_ref[at * slots + slot] = place


def add_products(slots, inner_local, places_ref, a_refs, a_owners, b_refs, b_owners, total):
    cells = (total.shape[0] // BS - 1) * inner_local
    depth = b_refs[0].shape[0] // BS
    groups = []
    for at, (a_ref, owner) in enumerate(zip(a_refs, a_owners)):
        places = [places_ref[at * slots + slot] for slot in range(slots)]
        if inner_local == 1:
            groups.append((a_ref, 0, places, owner))
        else:
            for slot, place in enumerate(places):
                inside = jnp.where(place < cells, lax.rem(place, inner_local), 0)
                groups.append((a_ref, slot, [place // inner_local], owner * inner_local + inside))
    for a_ref, slot, places, inner in groups:
        for b_ref, owner in zip(b_refs, b_owners):

            @pl.when((inner // depth if depth > 1 else inner) == owner)
            def _():
                inside = block(lax.rem(inner, depth)) if depth > 1 else slice(None)
                products = jnp.dot(
                    a_ref[pl.ds(slot * BS, len(places) * BS), :],
                    b_ref[inside, :],
                    preferred_element_type=jnp.float32,
                )
                for at, row in enumerate(places):
                    total[block(row), :] += products[at * BS : (at + 1) * BS]


def early_kernel(slots, inner_local, a_of, b_of, *refs):
    a_refs, b_refs = refs[: len(a_of)], refs[len(a_of) : -2]
    total, places_ref = refs[-2:]
    total[...] = jnp.zeros_like(total)
    read_places(slots, a_refs, places_ref)
    a_owners = [of(lax.axis_index("col")) for of in a_of]
    b_owners = [of(lax.axis_index("row")) for of in b_of]
    add_products(slots, inner_local, places_ref, a_refs, a_owners, b_refs, b_owners, total)


def late_kernel(slots, inner_local, a_of, b_of, total_ref, places_ref, *refs):
    a_refs, b_refs = refs[: len(a_of)], refs[len(a_of) : -4]
    total, out_ref, stage, sem = refs[-4:]
    a_owners = [of(lax.axis_index("col")) for of in a_of]
    b_owners = [of(lax.axis_index("row")) for of in b_of]
    add_products(slots, inner_local, places_ref, a_refs, a_owners, b_refs, b_owners, total)
    copies = []
    for row in range(out_ref.shape[0] // BS):
        stage[block(row), :] = total[block(row), :].astype(jnp.bfloat16)
        copies.append(
            pltpu.make_async_copy(stage.at[block(row), :], out_ref.at[block(row), :], sem.at[row])
        )
        copies[-1].start()
    for copy in copies:
        copy.wait()


def flip(step):
    return lambda me: me ^ step


def behind(step, n):
    return lambda me: lax.rem(me + n - step, n)


def route(n):
    own = list(range(n))
    if n & (n - 1):
        steps = [([(i, (i + s) % n) for i in own], None, s > n // 2) for s in range(1, n)]
    else:
        order = list(range(n // 2, n)) + list(range(1, n // 2))
        steps = [([(i, i ^ s) for i in own], None, at in LATE) for at, s in enumerate(order)]
    plan = []
    for pairs, source, late in steps:
        holds = {i: i for i in own} if source is None else plan[source][2]
        plan.append((pairs, source, {dst: holds[src] for src, dst in pairs}, late))
    return plan


def owner_of(table):
    def of(me):
        owner = jnp.int32(-1)
        for device, held in table.items():
            owner = jnp.where(me == device, held, owner)
        return owner

    return of


def spread(values, axis, n):
    same = lambda me: me
    held = [(values, same)]
    if n & (n - 1):
        return held + [
            (lax.ppermute(values, axis, [(i, (i + s) % n) for i in range(n)]), behind(s, n))
            for s in range(1, n)
        ]
    step = n // 2
    masks = [(values, 0)]
    while step:
        pairs = [(i, i ^ step) for i in range(n)]
        fresh = []
        for v, mask in masks:
            fresh.append((lax.ppermute(v, axis, pairs), mask ^ step))
        masks += fresh
        step //= 2
    return [(v, flip(mask)) for v, mask in masks]


VMEM = pl.BlockSpec(memory_space=pltpu.VMEM)
SMEM = pl.BlockSpec(memory_space=pltpu.SMEM)
HBM = pl.BlockSpec(memory_space=pltpu.HBM)


def per_device(shape, a_blocks, a_mask, b_blocks, b_mask):
    row_n, col_n = shape["row"], shape["col"]
    own_width = b_blocks.shape[1] // shape["rep"]
    depth = b_blocks.shape[0]
    rows = a_blocks.shape[0]
    block_rows, inner_local = a_mask.shape
    slots = max(block_rows // 4, 1)
    code_rows = -(-slots // CODE_ALIGN) * CODE_ALIGN
    packed, own_b = pl.pallas_call(
        functools.partial(prep_kernel, slots, block_rows, inner_local),
        out_shape=[
            pltpu.VMEM((slots * BS + code_rows, BS), jnp.bfloat16),
            pltpu.VMEM((depth, own_width), jnp.bfloat16),
        ],
        in_specs=[HBM] * 4,
        out_specs=[VMEM] * 2,
        scratch_shapes=[
            pltpu.SMEM(a_mask.shape[::-1], jnp.int32),
            pltpu.SMEM(b_mask.shape, jnp.int32),
            pltpu.VMEM(a_blocks.shape, jnp.bfloat16),
            pltpu.SemaphoreType.DMA,
            pltpu.SemaphoreType.DMA,
            pltpu.SemaphoreType.DMA((2,)),
        ],
        compiler_params=pltpu.CompilerParams(vmem_limit_bytes=60 << 20),
        name="prep",
    )(a_mask.T, a_blocks, b_mask, b_blocks)
    plan = route(row_n)
    arrived = []
    for pairs, source, _, _ in plan:
        sent = own_b if source is None else arrived[source]
        arrived.append(lax.ppermute(sent, "row", pairs))
    a_held = spread(packed, "col", col_n)
    held = [(v, owner_of(step[2]), step[3]) for v, step in zip(arrived, plan)]
    early = [(own_b, lambda me: me)] + [(v, of) for v, of, late in held if not late]
    late = [(v, of) for v, of, late in held if late]
    a_of = [of for _, of in a_held]
    total, places = pl.pallas_call(
        functools.partial(early_kernel, slots, inner_local, a_of, [of for _, of in early]),
        out_shape=[
            jax.ShapeDtypeStruct((rows + BS, own_width), jnp.float32),
            pltpu.SMEM((len(a_held) * slots,), jnp.int32),
        ],
        in_specs=[VMEM] * (len(a_held) + len(early)),
        out_specs=[VMEM, SMEM],
        compiler_params=pltpu.CompilerParams(vmem_limit_bytes=8 << 20),
        cost_estimate=pl.CostEstimate(flops=1 << 30, bytes_accessed=1 << 22, transcendentals=0),
        name="early",
    )(*[v for v, _ in a_held], *[v for v, _ in early])
    _, product = pl.pallas_call(
        functools.partial(late_kernel, slots, inner_local, a_of, [of for _, of in late]),
        out_shape=[
            jax.ShapeDtypeStruct((rows + BS, own_width), jnp.float32),
            jax.ShapeDtypeStruct((rows, own_width), jnp.bfloat16),
        ],
        in_specs=[VMEM, SMEM] + [VMEM] * (len(a_held) + len(late)),
        out_specs=[VMEM, HBM],
        scratch_shapes=[
            pltpu.VMEM((rows, own_width), jnp.bfloat16),
            pltpu.SemaphoreType.DMA((rows // BS,)),
        ],
        input_output_aliases={0: 0},
        compiler_params=pltpu.CompilerParams(vmem_limit_bytes=8 << 20),
        name="late",
    )(total, places, *[v for v, _ in a_held], *[v for v, _ in late])
    return product


def solution(mesh):
    in_specs = (P("row", "col"), P("row", "col"), P("row", "col"), P("row", "col"))
    out_specs = P("row", ("col", "rep"))
    return jax.shard_map(
        functools.partial(per_device, dict(mesh.shape)),
        mesh=mesh,
        in_specs=in_specs,
        out_specs=out_specs,
        check_vma=False,
    )
```
